32 devices in a mesh: gx: 16 (over z, x, core), gy: 2 (over y).
Axes of the slice: x: 2, y: 2, z: 4, core: 2. Of those that a mesh axis runs over, the one named last changes fastest.
Arguments:
- positions: float32 [3, 12, 32, 32, 256], P(None, None, 'gx', 'gy'), may hold values from 0 to 1
- velocities: float32 [3, 12, 32, 32, 256], P(None, None, 'gx', 'gy'), may hold values from -6 to 6
- thermal: float32 [3, 12, 32, 32, 256], P(None, None, 'gx', 'gy'), may hold values from -6 to 6
- offsets: int32 [12, 32, 32, 256], P(None, 'gx', 'gy'), may hold values from 0 to 7
- occupancy: int32 [12, 32, 32, 256], P(None, 'gx', 'gy'), may hold values from 0 to 1, as said below
- shift_codes: int32 [3], replicated, may hold values from 0 to 7
Outputs:
- new_velocities: float32 [3, 12, 32, 32, 256], P(None, None, 'gx', 'gy')
The draws below stay inside these ranges and needn't reach their ends.
Inputs may be any that keep to these rules, and one draw needn't show every extreme that they name: `occupancy`: the particles of a storage cell occupy its first slots; every storage cell holds 8 to 12 particles.
All inputs are finite; a program needn't handle non-finite values.
Results may differ from the reference program's by a relative error of at most 0.0001.
Values sent between devices are 32-bit elements; how exact they have to be, the bound alone decides.
A program may use at most 64 MiB of HBM per device.

```python
import jax
import jax.numpy as jnp

CZ = 256
SLOTS = 12
STEPS = 3
NX = 32
NY = 32


def draw_occupancy(key, part):
    counts = jax.random.randint(key, (1, NX, NY, CZ), SLOTS - 4, SLOTS + 1)
    slot_ids = jnp.arange(SLOTS, dtype=jnp.int32).reshape(SLOTS, 1, 1, 1)
    return (slot_ids < counts).astype(jnp.int32)


def touch_ends(drawn, own_key, least, largest):
    longest = drawn.shape.index(max(drawn.shape))
    spots = []
    for shift in (0, 1):
        where = [jax.random.randint(jax.random.fold_in(own_key, axis), (), 0, length) for axis, length in enumerate(drawn.shape)]
        where[longest] = (where[longest] + shift) % drawn.shape[longest]
        spots.append(tuple(where))
    return drawn.at[spots[0]].set(least).at[spots[1]].set(largest)


def levels(key, shape, cuts, least, largest):
    gain = 1.0
    for axis_at, blocks in cuts:
        draws = jax.random.uniform(jax.random.fold_in(jax.random.fold_in(key, 6), axis_at), (blocks,), jnp.float32, least / len(cuts), largest / len(cuts))
        gain = gain * jnp.repeat(jnp.exp(draws), shape[axis_at] // blocks).reshape((-1,) + (1,) * (len(shape) - 1 - axis_at))
    return gain


def bell_draw(own_key, extent, scale, reach, cuts=(), kind=jnp.bfloat16):
    gain = levels(own_key, extent, cuts, -0.22, 0.18) if cuts else 1.0
    drawn = jax.random.normal(own_key, extent, jnp.float32) * scale * gain
    return jnp.minimum(jnp.maximum(drawn, -reach), reach).astype(kind)


def setup_inputs(seed: int = 0) -> dict:
    splits = jax.random.split(jax.random.key(seed), 7)
    positions = jnp.clip(1.0 * jax.random.uniform(splits[0], (3, SLOTS, NX, NY, CZ), jnp.float32) ** levels(splits[0], (3, SLOTS, NX, NY, CZ), ((2, 16), (3, 2)), -0.2, 0.2), 0.0, 1.0)
    velocities = bell_draw(splits[1], (3, SLOTS, NX, NY, CZ), 1.0, 6.0, ((2, 16), (3, 2)), jnp.float32)
    thermal = bell_draw(splits[2], (3, SLOTS, NX, NY, CZ), 1.0, 6.0, ((2, 16), (3, 2)), jnp.float32)
    offsets = touch_ends(jax.random.randint(splits[3], (SLOTS, NX, NY, CZ), 0, 8), jax.random.fold_in(splits[3], 1), 0, 7).astype(jnp.int32)
    occupancy = draw_occupancy(jax.random.fold_in(splits[6], 71), 0)
    shift_codes = jax.random.randint(splits[5], (STEPS,), 0, 8).astype(jnp.int32)
    return dict(positions=positions, velocities=velocities, thermal=thermal, offsets=offsets, occupancy=occupancy, shift_codes=shift_codes)


ridge = 0.5


def offset_bits(code_value):
    return code_value // 4, (code_value // 2) % 2, code_value % 2


def cross_product(first, second):
    return [first[1] * second[2] - first[2] * second[1],
            first[2] * second[0] - first[0] * second[2],
            first[0] * second[1] - first[1] * second[0]]


def code_moments(positions, velocities, thermal, offsets, occupancy, code_value):
    shift_x, shift_y, shift_z = offset_bits(code_value)
    weight = jnp.where(offsets == code_value, occupancy, 0).astype(jnp.float32)
    shifted = [positions[0] + shift_x, positions[1] + shift_y, positions[2] + shift_z]
    relative = [velocities[component] - thermal[component] for component in range(3)]
    spins = cross_product(shifted, relative)
    seconds = [shifted[0] * shifted[0], shifted[1] * shifted[1], shifted[2] * shifted[2],
               shifted[0] * shifted[1], shifted[0] * shifted[2], shifted[1] * shifted[2]]
    terms = shifted + relative + spins + seconds
    return jnp.stack([jnp.sum(weight, axis=0)] + [jnp.sum(weight * term, axis=0) for term in terms])


def cell_solution(sums):
    count = jnp.maximum(sums[0], 1.0)
    first = [sums[1], sums[2], sums[3]]
    flow = [sums[4], sums[5], sums[6]]
    centre = [value / count for value in first]
    drift = [value / count for value in flow]
    moment = cross_product(centre, flow)
    torque = [sums[7 + component] - moment[component] for component in range(3)]
    mxx = sums[10] - first[0] * first[0] / count
    myy = sums[11] - first[1] * first[1] / count
    mzz = sums[12] - first[2] * first[2] / count
    mxy = sums[13] - first[0] * first[1] / count
    mxz = sums[14] - first[0] * first[2] / count
    myz = sums[15] - first[1] * first[2] / count
    trace = mxx + myy + mzz
    kxx = trace - mxx + ridge
    kyy = trace - myy + ridge
    kzz = trace - mzz + ridge
    kxy = -mxy
    kxz = -mxz
    kyz = -myz
    adj_xx = kyy * kzz - kyz * kyz
    adj_yy = kxx * kzz - kxz * kxz
    adj_zz = kxx * kyy - kxy * kxy
    adj_xy = kxz * kyz - kxy * kzz
    adj_xz = kxy * kyz - kxz * kyy
    adj_yz = kxy * kxz - kxx * kyz
    determinant = kxx * adj_xx + kxy * adj_xy + kxz * adj_xz
    spin_x = (adj_xx * torque[0] + adj_xy * torque[1] + adj_xz * torque[2]) / determinant
    spin_y = (adj_xy * torque[0] + adj_yy * torque[1] + adj_yz * torque[2]) / determinant
    spin_z = (adj_xz * torque[0] + adj_yz * torque[1] + adj_zz * torque[2]) / determinant
    return jnp.stack(centre + drift + [spin_x, spin_y, spin_z])


def particle_update(table, positions, thermal, offsets, occupancy, code_value, total):
    shift_x, shift_y, shift_z = offset_bits(code_value)
    shifted = [positions[0] + shift_x, positions[1] + shift_y, positions[2] + shift_z]
    arm = [shifted[component] - table[component] for component in range(3)]
    turn = cross_product([table[6], table[7], table[8]], arm)
    fresh = jnp.stack([thermal[component] + table[3 + component] + turn[component] for component in range(3)])
    keep = (offsets == code_value) & (occupancy == 1)
    return total + jnp.where(keep, fresh, jnp.zeros_like(fresh))


def one_collision(positions, velocities, thermal, offsets, occupancy):
    cell_sums = jnp.zeros((16,) + offsets.shape[1:], jnp.float32)
    for code_value in range(8):
        shift_x, shift_y, shift_z = offset_bits(code_value)
        partial_sums = code_moments(positions, velocities, thermal, offsets, occupancy, code_value)
        cell_sums = cell_sums + jnp.roll(partial_sums, (-shift_x, -shift_y, -shift_z), axis=(1, 2, 3))
    state = cell_solution(cell_sums)
    result = jnp.zeros(positions.shape, jnp.float32)
    for code_value in range(8):
        shift_x, shift_y, shift_z = offset_bits(code_value)
        table = jnp.roll(state, (shift_x, shift_y, shift_z), axis=(1, 2, 3))
        result = particle_update(table, positions, thermal, offsets, occupancy, code_value, result)
    return result


def reference(positions, velocities, thermal, offsets, occupancy, shift_codes):
    current = velocities
    for step_index in range(STEPS):
        codes = jnp.bitwise_xor(offsets, shift_codes[step_index])
        hot = jnp.roll(thermal, -step_index, axis=1)
        current = one_collision(positions, current, hot, codes, occupancy)
    return current
```

```python
import functools

import jax
import jax.numpy as jnp
from jax import lax
from jax.experimental import pallas as pl
from jax.experimental.pallas import tpu as pltpu
from jax.sharding import PartitionSpec as P

STEPS = 3
RIDGE = 0.5
F32 = jnp.float32
NS = 10
ND = 6
DIRS = ((-1, 0), (1, 0), (0, -1), (0, 1), (-1, -1), (-1, 1), (1, -1), (1, 1))


def pad8(v):
    return (v + 7) // 8 * 8


def cross(a, b):
    return [
        a[1] * b[2] - a[2] * b[1],
        a[2] * b[0] - a[0] * b[2],
        a[0] * b[1] - a[1] * b[0],
    ]


def translate_static(m, axis):
    n, x, y, z, xx, yy, zz, xy, xz, yz = m
    if axis == 0:
        return [n, x + n, y, z, xx + (x + x) + n, yy, zz, xy + y, xz + z, yz]
    if axis == 1:
        return [n, x, y + n, z, xx, yy + (y + y) + n, zz, xy + x, xz, yz + z]
    return [n, x, y, z + n, xx, yy, zz + (z + z) + n, xy, xz + x, yz + y]


def translate_dynamic(m, axis):
    wx, wy, wz, lx, ly, lz = m
    if axis == 0:
        return [wx, wy, wz, lx, ly - wz, lz + wy]
    if axis == 1:
        return [wx, wy, wz, lx + wz, ly, lz - wx]
    return [wx, wy, wz, lx - wy, ly + wx, lz]


def kernel(
    shift_h, pos_h, vel_h, th_h, off_h, occ_h, res,
    shift_ref, pos, vel, th, off, occ, grp, upd, est, edy,
    sx_s, sy_s, rx_s, ry_s, rc_s, sx_d, sy_d, rx_d, ry_d, rc_d,
    in_sem, send_sem, recv_sem,
):
    slots, rows, cols, depth = off.shape
    gx, gy = lax.axis_index("gx"), lax.axis_index("gy")
    nx, ny = lax.axis_size("gx"), lax.axis_size("gy")

    def device(dx, dy):
        return (lax.rem(gx + dx + nx, nx), lax.rem(gy + dy + ny, ny))

    loads = [
        pltpu.make_async_copy(src, dst, in_sem.at[k])
        for k, (src, dst) in enumerate(
            ((off_h, off), (occ_h, occ), (pos_h, pos), (th_h, th), (vel_h, vel), (shift_h, shift_ref))
        )
    ]
    for copy in loads:
        copy.start()
    barrier = pltpu.get_barrier_semaphore()
    for dx, dy in DIRS:
        pl.semaphore_signal(
            barrier, inc=1, device_id=device(dx, dy), device_id_type=pl.DeviceIdType.MESH
        )

    yb, zb = cols // 8, depth // 128
    blocks = rows * yb * zb
    code_ids = lax.broadcasted_iota(jnp.int32, (8, 8, 128), 0)

    def place(index):
        r = index // (yb * zb)
        rest = index % (yb * zb)
        y = pl.multiple_of((rest // zb) * 8, 8)
        z = pl.multiple_of((rest % zb) * 128, 128)
        return r, pl.ds(y, 8), pl.ds(z, 128)

    def accumulate(where_at, base, make_terms):
        r, ys, zs = where_at
        total = None
        for m in range(slots):
            mask = code_ids == off[m, r, ys, zs][None]
            terms = make_terms(m)
            picked = [jnp.where(mask, t if isinstance(t, float) else t[None], 0.0) for t in terms]
            total = picked if total is None else [a + b for a, b in zip(total, picked)]
        for k, value in enumerate(total):
            grp[base + k, :, r, ys, zs] = value

    def point(m, at):
        return [pos[(k, m) + at] for k in range(3)]

    for copy in loads[:3]:
        copy.wait()

    def static_block(index, carry):
        at = place(index)
        r, ys, zs = at
        for m in range(slots):
            off[m, r, ys, zs] = jnp.where(occ[m, r, ys, zs] == 1, off[m, r, ys, zs], 8)
        accumulate(at, 0, lambda m: [1.0] + point(m, at))

        def squares(m):
            return [v * v for v in point(m, at)]

        def products(m):
            x, y, z = point(m, at)
            return [x * y, x * z, y * z]

        accumulate(at, 4, squares)
        accumulate(at, 7, products)
        return carry

    def flow_block(step, index, carry):
        at = place(index)

        def flow(m):
            now = [th[(k, (m + step) % slots) + at] for k in range(3)]
            if step == 0:
                before = [vel[(k, m) + at] for k in range(3)]
            else:
                before = [th[(k, (m + step - 1) % slots) + at] for k in range(3)]
            return [a - b for a, b in zip(before, now)]

        accumulate(at, NS + ND * step, flow)
        accumulate(at, NS + ND * step + 3, lambda m: cross(point(m, at), flow(m)))
        return carry

    sub = lax.broadcasted_iota(jnp.int32, (cols, depth), 0)

    def build(load, translate, count, ext, sx, sy):
        vp = pad8(count)

        def merged(e, by):
            halves = []
            for bz in range(2):
                parts = []
                if e > 0:
                    parts.append(load(2 * by + bz, e - 1))
                if e < rows:
                    parts.append(translate(load(4 + 2 * by + bz, e), 0))
                halves.append(parts[0] if len(parts) == 1 else [a + b for a, b in zip(*parts)])
            high = [pltpu.roll(v, depth - 1, 1) for v in translate(halves[1], 2)]
            return [a + b for a, b in zip(halves[0], high)]

        for e in range(rows + 1):
            low = merged(e, 0)
            high = translate(merged(e, 1), 1)
            for v in range(count):
                moved = pltpu.roll(high[v], cols - 1, 0)
                main = low[v] + jnp.where(sub == cols - 1, 0.0, moved)
                rim = high[v][0:1]
                ext[v, e, 0:cols] = main
                ext[v, e, cols : cols + 1] = rim
                for side, row in ((0, 0), (1, rows)):
                    if e == row:
                        sx[side, v * cols : (v + 1) * cols] = main
                        sx[side, count * cols + v : count * cols + v + 1] = rim
                sy[0, e * vp + v : e * vp + v + 1] = rim
                sy[1, e * vp + v : e * vp + v + 1] = main[cols - 1 : cols]

    def copies(count, sx, sy, rx, ry, rc, kind, step):
        vp = pad8(count)
        out = []
        for k, (dx, dy) in enumerate(DIRS):
            if dy == 0:
                src, dst = sx.at[k], rx.at[k]
            elif dx == 0:
                src, dst = sy.at[k - 2], ry.at[k - 2]
            else:
                src = sy.at[0 if dy < 0 else 1, pl.ds((0 if dx < 0 else rows) * vp, vp)]
                dst = rc.at[k - 4]
            out.append(
                pltpu.make_async_remote_copy(
                    src_ref=src, dst_ref=dst,
                    send_sem=send_sem.at[kind, step, k],
                    recv_sem=recv_sem.at[kind, step, k],
                    device_id=device(dx, dy),
                    device_id_type=pl.DeviceIdType.MESH,
                )
            )
        return out

    def absorb(count, ext, rx, ry, rc, sent):
        vp = pad8(count)
        for copy in sent:
            copy.wait_recv()
        for v in range(count):
            for side, e in ((0, rows), (1, 0)):
                ext[v, e, 0:cols] += rx[side, v * cols : (v + 1) * cols]
                ext[v, e, cols : cols + 1] += rx[side, count * cols + v : count * cols + v + 1]
            for e in range(rows + 1):
                for side, row in ((0, cols - 1), (1, cols)):
                    extra = ry[side, e * vp + v : e * vp + v + 1]
                    if e == rows:
                        extra = extra + rc[side, v : v + 1]
                    if e == 0:
                        extra = extra + rc[2 + side, v : v + 1]
                    ext[v, e, row : row + 1] += extra

    def static_solve(ext):
        for e in range(rows + 1):
            n, sx, sy, sz, xx, yy, zz, xy, xz, yz = [ext[v, e] for v in range(NS)]
            inv = 1.0 / jnp.maximum(n, 1.0)
            cx, cy, cz = sx * inv, sy * inv, sz * inv
            mxx, myy, mzz = xx - sx * cx, yy - sy * cy, zz - sz * cz
            kxy, kxz, kyz = sx * cy - xy, sx * cz - xz, sy * cz - yz
            kxx = myy + mzz + RIDGE
            kyy = mxx + mzz + RIDGE
            kzz = mxx + myy + RIDGE
            axx = kyy * kzz - kyz * kyz
            ayy = kxx * kzz - kxz * kxz
            azz = kxx * kyy - kxy * kxy
            axy = kxz * kyz - kxy * kzz
            axz = kxy * kyz - kxz * kyy
            ayz = kxy * kxz - kxx * kyz
            scale = 1.0 / (kxx * axx + kxy * axy + kxz * axz)
            done = [inv, cx, cy, cz] + [a * scale for a in (axx, ayy, azz, axy, axz, ayz)]
            for v in range(NS):
                ext[v, e] = done[v]

    def tables(ext, dyn):
        out = []
        for e in range(rows + 1):
            inv, cx, cy, cz, ixx, iyy, izz, ixy, ixz, iyz = [ext[v, e] for v in range(NS)]
            flow = [dyn[v, e] for v in range(3)]
            centre = [cx, cy, cz]
            tq = [dyn[3 + k, e] - t for k, t in enumerate(cross(centre, flow))]
            spin = [
                ixx * tq[0] + ixy * tq[1] + ixz * tq[2],
                ixy * tq[0] + iyy * tq[1] + iyz * tq[2],
                ixz * tq[0] + iyz * tq[1] + izz * tq[2],
            ]
            base = [f * inv - t for f, t in zip(flow, cross(spin, centre))]
            by_bits = {}
            values = base + spin
            straight = [v[0:cols] for v in values]
            moved = [
                jnp.where(
                    sub == 0,
                    jnp.broadcast_to(v[cols : cols + 1], (cols, depth)),
                    pltpu.roll(v[0:cols], 1, 0),
                )
                for v in values
            ]
            for by, plain in ((0, straight), (1, moved)):
                by_bits[by, 0] = plain
                by_bits[by, 1] = [pltpu.roll(v, 1, 1) for v in plain]
            out.append(by_bits)
        return out

    def solve(step):
        made = tables(est.at[step], edy)
        shift = shift_ref[step]
        for code in range(8):
            bits = (code // 4, code // 2 % 2, code % 2)
            for r in range(rows):
                a0, a1, a2, s0, s1, s2 = made[r - bits[0] + 1][bits[1], bits[2]]
                if bits[2]:
                    a0, a1 = a0 + s1, a1 - s0
                if bits[1]:
                    a0, a2 = a0 - s2, a2 + s0
                if bits[0]:
                    a1, a2 = a1 + s2, a2 - s1
                if step == STEPS - 1:
                    done = [a0, a1, a2, s0, s1, s2]
                else:
                    own = jnp.bitwise_xor(shift, code)
                    n, x, y, z, xx, yy, zz, xy, xz, yz = [grp[v, own, r] for v in range(NS)]
                    turn = cross([s0, s1, s2], [x, y, z])
                    arm = cross([x, y, z], [a0, a1, a2])
                    done = [
                        n * a0 + turn[0],
                        n * a1 + turn[1],
                        n * a2 + turn[2],
                        arm[0] + (yy + zz) * s0 - xy * s1 - xz * s2,
                        arm[1] + (xx + zz) * s1 - xy * s0 - yz * s2,
                        arm[2] + (xx + yy) * s2 - xz * s0 - yz * s1,
                    ]
                for v in range(ND):
                    upd[v, code, r] = done[v]

    def load_static(step):
        shift = shift_ref[step]

        def load(code, r):
            own = jnp.bitwise_xor(shift, code)
            return [grp[v, own, r] for v in range(NS)]

        return load

    def load_dynamic(step):
        shift = shift_ref[step]

        def load(code, r):
            own = jnp.bitwise_xor(shift, code)
            values = [grp[NS + ND * step + v, own, r] for v in range(ND)]
            if step:
                last = jnp.bitwise_xor(own, shift_ref[step - 1])
                values = [a + upd[v, last, r] for v, a in enumerate(values)]
            return values

        return load

    static_sent = [
        copies(NS, sx_s.at[s], sy_s.at[s], rx_s.at[s], ry_s.at[s], rc_s.at[s], 0, s)
        for s in range(STEPS)
    ]
    dynamic_sent = [
        copies(ND, sx_d.at[s], sy_d.at[s], rx_d.at[s], ry_d.at[s], rc_d.at[s], 1, s)
        for s in range(STEPS)
    ]

    def send_static(s):
        build(load_static(s), translate_static, NS, est.at[s], sx_s.at[s], sy_s.at[s])
        for copy in static_sent[s]:
            copy.start()

    def send_dynamic(s):
        build(load_dynamic(s), translate_dynamic, ND, edy, sx_d.at[s], sy_d.at[s])
        for copy in dynamic_sent[s]:
            copy.start()

    def finish_static(s):
        absorb(NS, est.at[s], rx_s.at[s], ry_s.at[s], rc_s.at[s], static_sent[s])
        static_solve(est.at[s])

    lax.fori_loop(0, blocks, static_block, 0)
    pl.semaphore_wait(barrier, len(DIRS))
    loads[5].wait()
    send_static(0)
    for copy in loads[3:5]:
        copy.wait()
    lax.fori_loop(0, blocks, functools.partial(flow_block, 0), 0)
    send_dynamic(0)
    lax.fori_loop(0, blocks, functools.partial(flow_block, 1), 0)
    lax.fori_loop(0, blocks, functools.partial(flow_block, 2), 0)
    send_static(1)
    finish_static(0)
    for s in range(STEPS):
        absorb(ND, edy, rx_d.at[s], ry_d.at[s], rc_d.at[s], dynamic_sent[s])
        solve(s)
        if s + 1 < STEPS:
            send_dynamic(s + 1)
            if s == 0:
                send_static(2)
            finish_static(s + 1)

    shift = shift_ref[STEPS - 1]
    last_step = STEPS - 1

    def final_block(index, carry):
        at = place(index)
        r, ys, zs = at
        for first in range(0, slots, 6):
            batch = range(first, min(first + 6, slots))
            codes = {m: off[m, r, ys, zs] for m in batch}
            picked = {m: [] for m in batch}
            for v in range(ND):
                leaf = [upd[v, jnp.bitwise_xor(shift, o), r, ys, zs] for o in range(8)]
                for m in batch:
                    one = jnp.bitwise_and(codes[m], 1) == 1
                    two = jnp.bitwise_and(codes[m], 2) == 2
                    four = jnp.bitwise_and(codes[m], 4) == 4
                    level = [jnp.where(one, leaf[k + 1], leaf[k]) for k in range(0, 8, 2)]
                    level = [jnp.where(two, level[k + 1], level[k]) for k in range(0, 4, 2)]
                    picked[m].append(jnp.where(four, level[1], level[0]))
            for m in batch:
                turn = cross(picked[m][3:], point(m, at))
                full = codes[m] < 8
                for k in range(3):
                    hot = th[(k, (m + last_step) % slots) + at]
                    res[k, m, r, ys, zs] = jnp.where(full, hot + picked[m][k] + turn[k], 0.0)
        return carry

    lax.fori_loop(0, blocks, final_block, 0)
    for group in static_sent + dynamic_sent:
        for copy in group:
            copy.wait_send()


def local(positions, velocities, thermal, offsets, occupancy, shift_codes):
    args = (shift_codes, positions, velocities, thermal, offsets, occupancy)
    slots, rows, cols, depth = offsets.shape
    full = (3, slots, rows, cols, depth)
    plane = (slots, rows, cols, depth)

    def faces(count):
        vp = pad8(count)
        wide = pltpu.VMEM((STEPS, 2, count * cols + vp, depth), F32)
        thin = pltpu.VMEM((STEPS, 2, (rows + 1) * vp, depth), F32)
        return [wide, thin, wide, thin, pltpu.VMEM((STEPS, 4, vp, depth), F32)]

    hbm = pl.BlockSpec(memory_space=pltpu.HBM)
    return pl.pallas_call(
        kernel,
        out_shape=pltpu.VMEM(full, F32),
        in_specs=[hbm] * 6,
        out_specs=pl.BlockSpec(memory_space=pltpu.VMEM),
        scratch_shapes=[
            pltpu.SMEM((STEPS,), jnp.int32),
            pltpu.VMEM(full, F32),
            pltpu.VMEM(full, F32),
            pltpu.VMEM(full, F32),
            pltpu.VMEM(plane, jnp.int32),
            pltpu.VMEM(plane, jnp.int32),
            pltpu.VMEM((NS + ND * STEPS, 8, rows, cols, depth), F32),
            pltpu.VMEM((ND, 8, rows, cols, depth), F32),
            pltpu.VMEM((STEPS, NS, rows + 1, cols + 8, depth), F32),
            pltpu.VMEM((ND, rows + 1, cols + 8, depth), F32),
            *faces(NS),
            *faces(ND),
            pltpu.SemaphoreType.DMA((6,)),
            pltpu.SemaphoreType.DMA((2, STEPS, len(DIRS))),
            pltpu.SemaphoreType.DMA((2, STEPS, len(DIRS))),
        ],
        compiler_params=pltpu.CompilerParams(
            collective_id=0, has_side_effects=True, vmem_limit_bytes=40000000
        ),
    )(*[pltpu.with_memory_space_constraint(v, pltpu.HBM) for v in args])


def solution(mesh):
    in_specs = (
        P(None, None, "gx", "gy", None),
        P(None, None, "gx", "gy", None),
        P(None, None, "gx", "gy", None),
        P(None, "gx", "gy", None),
        P(None, "gx", "gy", None),
        P(),
    )
    out_specs = P(None, None, "gx", "gy", None)
    return jax.shard_map(local, mesh=mesh, in_specs=in_specs, out_specs=out_specs, check_vma=False)
```

```python
import functools

import jax
import jax.numpy as jnp
from jax import lax
from jax.experimental import pallas as pl
from jax.experimental.pallas import tpu as pltpu
from jax.sharding import PartitionSpec as P

STEPS = 3
RIDGE = 0.5
F32 = jnp.float32
NS = 10
ND = 6
DIRS = ((-1, 0), (1, 0), (0, -1), (0, 1), (-1, -1), (-1, 1), (1, -1), (1, 1))


def pad8(v):
    return (v + 7) // 8 * 8


def cross(a, b):
    return [
        a[1] * b[2] - a[2] * b[1],
        a[2] * b[0] - a[0] * b[2],
        a[0] * b[1] - a[1] * b[0],
    ]


def translate_static(m, axis):
    n, x, y, z, xx, yy, zz, xy, xz, yz = m
    if axis == 0:
        return [n, x + n, y, z, xx + (x + x) + n, yy, zz, xy + y, xz + z, yz]
    if axis == 1:
        return [n, x, y + n, z, xx, yy + (y + y) + n, zz, xy + x, xz, yz + z]
    return [n, x, y, z + n, xx, yy, zz + (z + z) + n, xy, xz + x, yz + y]


def translate_dynamic(m, axis):
    wx, wy, wz, lx, ly, lz = m
    if axis == 0:
        return [wx, wy, wz, lx, ly - wz, lz + wy]
    if axis == 1:
        return [wx, wy, wz, lx + wz, ly, lz - wx]
    return [wx, wy, wz, lx - wy, ly + wx, lz]


def kernel(
    shift_h, pos_h, vel_h, th_h, off_h, occ_h, res,
    shift_ref, pos, vel, th, off, occ, code, grp, upd, made, est, edy,
    sx_s, sy_s, sc_s, rx_s, ry_s, rc_s, sx_d, sy_d, sc_d, rx_d, ry_d, rc_d,
    in_sem, row_sem, send_sem, recv_sem,
):
    slots, rows, cols, depth = off.shape
    gx, gy = lax.axis_index("gx"), lax.axis_index("gy")
    nx, ny = lax.axis_size("gx"), lax.axis_size("gy")

    def device(dx, dy):
        return (lax.rem(gx + dx + nx, nx), lax.rem(gy + dy + ny, ny))

    shift_load = pltpu.make_async_copy(shift_h, shift_ref, in_sem.at[0])
    shift_load.start()
    lead = lax.rem(gx, 2)
    lead_row, lead_half, lead_edge = lead * (rows - 1), 1 - lead, lead * rows
    tail_row, tail_half, tail_edge = rows - 1 - lead_row, lead, rows - lead_edge
    loads = []
    for k, r in enumerate([lead_row, tail_row][: min(rows, 2)] + list(range(1, rows - 1))):
        pairs = (
            (off_h.at[:, r], off.at[:, r]),
            (occ_h.at[:, r], occ.at[:, r]),
            (pos_h.at[:, :, r], pos.at[:, :, r]),
            (th_h.at[:, :, r], th.at[:, :, r]),
            (vel_h.at[:, :, r], vel.at[:, :, r]),
        )
        loads.append(
            [pltpu.make_async_copy(a, b, row_sem.at[k, i]) for i, (a, b) in enumerate(pairs)]
        )
        for copy in loads[k]:
            copy.start()

    def wait_loads(wanted):
        for copy in wanted:
            copy.wait()

    barrier = pltpu.get_barrier_semaphore()
    for dx, dy in DIRS:
        pl.semaphore_signal(
            barrier, inc=1, device_id=device(dx, dy), device_id_type=pl.DeviceIdType.MESH
        )

    yb, zb = cols // 8, depth // 128
    blocks = yb * zb
    edges = [(0, 1), (rows - 1, 0)]
    second = [(r, h) for r in range(rows) for h in range(2) if (r, h) not in edges]

    def place(r, index):
        y = pl.multiple_of((index // zb) * 8, 8)
        z = pl.multiple_of((index % zb) * 128, 128)
        return r, pl.ds(y, 8), pl.ds(z, 128)

    def accumulate(at, base, wanted, make_terms, new=False):
        total = None
        for m in range(slots):
            if new:
                moved = jnp.bitwise_xor(off[(m,) + at], shift_ref[0])
                own = jnp.where(occ[(m,) + at] == 1, moved, 8)
                code[(m,) + at] = own
            else:
                own = code[(m,) + at]
            terms = make_terms(m)
            picked = []
            for c in wanted:
                mask = own == c
                picked.append([jnp.where(mask, t, 0.0) for t in terms])
            if total is None:
                total = picked
            else:
                total = [[a + b for a, b in zip(u, v)] for u, v in zip(total, picked)]
        for c, values in zip(wanted, total):
            for k, value in enumerate(values):
                grp[(base + k, c) + at] = value

    def point(m, at):
        return [pos[(k, m) + at] for k in range(3)]

    def codes_of(h):
        return [4 * h + c for c in range(4)]

    def shifted(s):
        return jnp.bitwise_xor(shift_ref[s], shift_ref[0])

    def static_sums(r, h, new=False):
        def body(index, carry):
            at = place(r, index)

            def terms(m):
                x, y, z = point(m, at)
                return [1.0, x, y, z, x * x, y * y, z * z, x * y, x * z, y * z]

            accumulate(at, 0, codes_of(h), terms, new)
            return carry

        lax.fori_loop(0, blocks, body, 0)

    def flow_sums(step, r, wanted):
        def body(index, carry):
            at = place(r, index)

            def terms(m):
                now = [th[(k, (m + step) % slots) + at] for k in range(3)]
                if step == 0:
                    before = [vel[(k, m) + at] for k in range(3)]
                else:
                    before = [th[(k, (m + step - 1) % slots) + at] for k in range(3)]
                flow = [a - b for a, b in zip(before, now)]
                return flow + cross(point(m, at), flow)

            accumulate(at, NS + ND * step, wanted, terms)
            return carry

        lax.fori_loop(0, blocks, body, 0)

    sub = lax.broadcasted_iota(jnp.int32, (cols, depth), 0)

    def build(load, translate, count, ext, sx, sy, sc, edges):
        def merged(e, by):
            halves = []
            for bz in range(2):
                parts = []
                if e > 0:
                    parts.append(load(2 * by + bz, e - 1))
                if e < rows:
                    parts.append(translate(load(4 + 2 * by + bz, e), 0))
                halves.append(parts[0] if len(parts) == 1 else [a + b for a, b in zip(*parts)])
            high = [pltpu.roll(v, depth - 1, 1) for v in translate(halves[1], 2)]
            return [a + b for a, b in zip(halves[0], high)]

        for e in edges:
            low = merged(e, 0)
            high = translate(merged(e, 1), 1)
            for v in range(count):
                moved = pltpu.roll(high[v], cols - 1, 0)
                main = low[v] + jnp.where(sub == cols - 1, 0.0, moved)
                rim, last = high[v][0:1], main[cols - 1 : cols]
                ext[v, e, 0:cols] = main
                ext[v, e, cols : cols + 1] = rim
                for side, row in ((0, 0), (1, rows)):
                    if e == row:
                        sx[side, v * cols : (v + 1) * cols] = main
                        sx[side, count * cols + v : count * cols + v + 1] = rim
                        sc[2 * side, v : v + 1] = rim
                        sc[2 * side + 1, v : v + 1] = last
                sy[0, e * count + v : e * count + v + 1] = rim
                sy[1, e * count + v : e * count + v + 1] = last

    def copies(sx, sy, sc, rx, ry, rc, kind, step):
        out = []
        for k, (dx, dy) in enumerate(DIRS):
            if dy == 0:
                src, dst = sx.at[k], rx.at[k]
            elif dx == 0:
                src, dst = sy.at[k - 2], ry.at[k - 2]
            else:
                src, dst = sc.at[k - 4], rc.at[k - 4]
            out.append(
                pltpu.make_async_remote_copy(
                    src_ref=src, dst_ref=dst,
                    send_sem=send_sem.at[kind, step, k],
                    recv_sem=recv_sem.at[kind, step, k],
                    device_id=device(dx, dy),
                    device_id_type=pl.DeviceIdType.MESH,
                )
            )
        return out

    def absorb(count, ext, rx, ry, rc, sent):
        for copy in sent:
            copy.wait_recv()
        for v in range(count):
            for side, e in ((0, rows), (1, 0)):
                ext[v, e, 0:cols] += rx[side, v * cols : (v + 1) * cols]
                ext[v, e, cols : cols + 1] += rx[side, count * cols + v : count * cols + v + 1]
            for e in range(rows + 1):
                for side, row in ((0, cols - 1), (1, cols)):
                    extra = ry[side, e * count + v : e * count + v + 1]
                    if e == rows:
                        extra = extra + rc[side, v : v + 1]
                    if e == 0:
                        extra = extra + rc[2 + side, v : v + 1]
                    ext[v, e, row : row + 1] += extra

    def static_solve(ext):
        for e in range(rows + 1):
            n, sx, sy, sz, xx, yy, zz, xy, xz, yz = [ext[v, e] for v in range(NS)]
            inv = 1.0 / jnp.maximum(n, 1.0)
            cx, cy, cz = sx * inv, sy * inv, sz * inv
            mxx, myy, mzz = xx - sx * cx, yy - sy * cy, zz - sz * cz
            kxy, kxz, kyz = sx * cy - xy, sx * cz - xz, sy * cz - yz
            kxx = myy + mzz + RIDGE
            kyy = mxx + mzz + RIDGE
            kzz = mxx + myy + RIDGE
            axx = kyy * kzz - kyz * kyz
            ayy = kxx * kzz - kxz * kxz
            azz = kxx * kyy - kxy * kxy
            axy = kxz * kyz - kxy * kzz
            axz = kxy * kyz - kxz * kyy
            ayz = kxy * kxz - kxx * kyz
            scale = 1.0 / (kxx * axx + kxy * axy + kxz * axz)
            done = [inv, cx, cy, cz] + [a * scale for a in (axx, ayy, azz, axy, axz, ayz)]
            for v in range(NS):
                ext[v, e] = done[v]

    def table(ext, dyn, e):
        inv, cx, cy, cz, ixx, iyy, izz, ixy, ixz, iyz = [ext[v, e] for v in range(NS)]
        flow = [dyn[v, e] for v in range(3)]
        centre = [cx, cy, cz]
        tq = [dyn[3 + k, e] - t for k, t in enumerate(cross(centre, flow))]
        spin = [
            ixx * tq[0] + ixy * tq[1] + ixz * tq[2],
            ixy * tq[0] + iyy * tq[1] + iyz * tq[2],
            ixz * tq[0] + iyz * tq[1] + izz * tq[2],
        ]
        base = [f * inv - t for f, t in zip(flow, cross(spin, centre))]
        values = base + spin
        straight = [v[0:cols] for v in values]
        moved = [
            jnp.where(
                sub == 0,
                jnp.broadcast_to(v[cols : cols + 1], (cols, depth)),
                pltpu.roll(v[0:cols], 1, 0),
            )
            for v in values
        ]
        for by, plain in ((0, straight), (1, moved)):
            for v in range(ND):
                made[e, by, 0, v] = plain[v]
                made[e, by, 1, v] = pltpu.roll(plain[v], 1, 1)

    def solve_row(step, r):
        delta = shifted(step)
        for want in range(8):
            bits = (want // 4, want // 2 % 2, want % 2)
            a0, a1, a2, s0, s1, s2 = [
                made[r - bits[0] + 1, bits[1], bits[2], v] for v in range(ND)
            ]
            if bits[2]:
                a0, a1 = a0 + s1, a1 - s0
            if bits[1]:
                a0, a2 = a0 - s2, a2 + s0
            if bits[0]:
                a1, a2 = a1 + s2, a2 - s1
            if step == STEPS - 1:
                done = [a0, a1, a2, s0, s1, s2]
            else:
                own = jnp.bitwise_xor(delta, want)
                n, x, y, z, xx, yy, zz, xy, xz, yz = [grp[v, own, r] for v in range(NS)]
                turn = cross([s0, s1, s2], [x, y, z])
                arm = cross([x, y, z], [a0, a1, a2])
                done = [
                    n * a0 + turn[0],
                    n * a1 + turn[1],
                    n * a2 + turn[2],
                    arm[0] + (yy + zz) * s0 - xy * s1 - xz * s2,
                    arm[1] + (xx + zz) * s1 - xy * s0 - yz * s2,
                    arm[2] + (xx + yy) * s2 - xz * s0 - yz * s1,
                ]
            for v in range(ND):
                upd[v, want, r] = done[v]

    def load_static(step):
        delta = shifted(step)

        def load(want, r):
            own = want if step == 0 else jnp.bitwise_xor(delta, want)
            return [grp[v, own, r] for v in range(NS)]

        return load

    def load_dynamic(step):
        delta = shifted(step)

        def load(want, r):
            own = want if step == 0 else jnp.bitwise_xor(delta, want)
            values = [grp[NS + ND * step + v, own, r] for v in range(ND)]
            if step:
                last = jnp.bitwise_xor(own, shifted(step - 1))
                values = [a + upd[v, last, r] for v, a in enumerate(values)]
            return values

        return load

    static_sent = [
        copies(sx_s.at[s], sy_s.at[s], sc_s.at[s], rx_s.at[s], ry_s.at[s], rc_s.at[s], 0, s)
        for s in range(STEPS)
    ]
    dynamic_sent = [
        copies(sx_d.at[s], sy_d.at[s], sc_d.at[s], rx_d.at[s], ry_d.at[s], rc_d.at[s], 1, s)
        for s in range(STEPS)
    ]
    groups = {0: (0, 4, 5), rows: (1, 6, 7)}

    def send_edge(sent, e):
        for k in groups[e]:
            sent[k].start()

    def send_sides(sent):
        sent[2].start()
        sent[3].start()

    def build_static(s, edges):
        build(
            load_static(s), translate_static, NS, est.at[s],
            sx_s.at[s], sy_s.at[s], sc_s.at[s], edges,
        )

    def build_dynamic(s, edges):
        build(
            load_dynamic(s), translate_dynamic, ND, edy,
            sx_d.at[s], sy_d.at[s], sc_d.at[s], edges,
        )

    def send_static(s):
        for e in (0, rows):
            send_edge(static_sent[s], e)
        send_sides(static_sent[s])

    def finish_static(s):
        absorb(NS, est.at[s], rx_s.at[s], ry_s.at[s], rc_s.at[s], static_sent[s])
        static_solve(est.at[s])

    inner = range(1, rows)

    def at_edge(edge, act):
        for e in (0, rows):
            pl.when(edge == e)(functools.partial(act, e))

    def static_edge(s, e):
        build_static(s, [e])
        send_edge(static_sent[s], e)

    def dynamic_edge(s, e):
        build_dynamic(s, [e])
        send_edge(dynamic_sent[s], e)

    shift_load.wait()
    wait_loads(loads[0][:3])
    static_sums(lead_row, lead_half, True)
    pl.semaphore_wait(barrier, len(DIRS))
    at_edge(lead_edge, functools.partial(static_edge, 0))
    wait_loads(loads[0][3:])
    flow_sums(0, lead_row, codes_of(lead_half))
    at_edge(lead_edge, functools.partial(dynamic_edge, 0))
    for group in loads[1:]:
        wait_loads(group)
    static_sums(tail_row, tail_half, True)
    at_edge(tail_edge, functools.partial(static_edge, 0))
    flow_sums(0, tail_row, codes_of(tail_half))
    at_edge(tail_edge, functools.partial(dynamic_edge, 0))
    for r, h in second:
        static_sums(r, h, 0 < r < rows - 1 and h == 0)
    build_static(0, inner)
    send_sides(static_sent[0])
    for r, h in second:
        flow_sums(0, r, codes_of(h))
    build_dynamic(0, inner)
    send_sides(dynamic_sent[0])
    build_static(1, range(rows + 1))
    send_static(1)
    for r in range(rows):
        flow_sums(1, r, range(8))
    finish_static(0)
    for s in range(STEPS):
        absorb(ND, edy, rx_d.at[s], ry_d.at[s], rc_d.at[s], dynamic_sent[s])
        table(est.at[s], edy, lead_edge)
        for e in inner:
            table(est.at[s], edy, e)
        solve_row(s, lead_row)
        if s + 1 < STEPS:
            at_edge(lead_edge, functools.partial(dynamic_edge, s + 1))
        table(est.at[s], edy, tail_edge)
        if rows > 1:
            solve_row(s, tail_row)
        if s + 1 < STEPS:
            at_edge(tail_edge, functools.partial(dynamic_edge, s + 1))
        for r in range(1, rows - 1):
            solve_row(s, r)
        if s + 1 < STEPS:
            build_dynamic(s + 1, inner)
            send_sides(dynamic_sent[s + 1])
            if s == 0:
                build_static(2, range(rows + 1))
                for r in range(rows):
                    flow_sums(2, r, range(8))
                send_static(2)
            finish_static(s + 1)

    last_delta = shifted(STEPS - 1)
    last_step = STEPS - 1

    def final_block(r, index, carry):
        at = place(r, index)
        for start in range(0, slots, 6):
            batch = range(start, min(start + 6, slots))
            codes = {m: code[(m,) + at] for m in batch}
            picked = {m: [] for m in batch}
            for v in range(ND):
                leaf = [upd[(v, jnp.bitwise_xor(last_delta, o)) + at] for o in range(8)]
                for m in batch:
                    one = jnp.bitwise_and(codes[m], 1) == 1
                    two = jnp.bitwise_and(codes[m], 2) == 2
                    four = jnp.bitwise_and(codes[m], 4) == 4
                    level = [jnp.where(one, leaf[k + 1], leaf[k]) for k in range(0, 8, 2)]
                    level = [jnp.where(two, level[k + 1], level[k]) for k in range(0, 4, 2)]
                    picked[m].append(jnp.where(four, level[1], level[0]))
            for m in batch:
                turn = cross(picked[m][3:], point(m, at))
                full = codes[m] < 8
                for k in range(3):
                    hot = th[(k, (m + last_step) % slots) + at]
                    res[(k, m) + at] = jnp.where(full, hot + picked[m][k] + turn[k], 0.0)
        return carry

    for r in range(rows):
        lax.fori_loop(0, blocks, functools.partial(final_block, r), 0)
    for group in static_sent + dynamic_sent:
        for copy in group:
            copy.wait_send()


def local(positions, velocities, thermal, offsets, occupancy, shift_codes):
    args = (shift_codes, positions, velocities, thermal, offsets, occupancy)
    slots, rows, cols, depth = offsets.shape
    full = (3, slots, rows, cols, depth)
    plane = (slots, rows, cols, depth)

    def faces(count):
        wide = pltpu.VMEM((STEPS, 2, count * cols + pad8(count), depth), F32)
        thin = pltpu.VMEM((STEPS, 2, pad8((rows + 1) * count), depth), F32)
        tips = pltpu.VMEM((STEPS, 4, pad8(count), depth), F32)
        return [wide, thin, tips] * 2

    hbm = pl.BlockSpec(memory_space=pltpu.HBM)
    return pl.pallas_call(
        kernel,
        out_shape=pltpu.VMEM(full, F32),
        in_specs=[hbm] * 6,
        out_specs=pl.BlockSpec(memory_space=pltpu.VMEM),
        scratch_shapes=[
            pltpu.SMEM((STEPS,), jnp.int32),
            pltpu.VMEM(full, F32),
            pltpu.VMEM(full, F32),
            pltpu.VMEM(full, F32),
            pltpu.VMEM(plane, jnp.int32),
            pltpu.VMEM(plane, jnp.int32),
            pltpu.VMEM(plane, jnp.int32),
            pltpu.VMEM((NS + ND * STEPS, 8, rows, cols, depth), F32),
            pltpu.VMEM((ND, 8, rows, cols, depth), F32),
            pltpu.VMEM((rows + 1, 2, 2, ND, cols, depth), F32),
            pltpu.VMEM((STEPS, NS, rows + 1, cols + 8, depth), F32),
            pltpu.VMEM((ND, rows + 1, cols + 8, depth), F32),
            *faces(NS),
            *faces(ND),
            pltpu.SemaphoreType.DMA((1,)),
            pltpu.SemaphoreType.DMA((rows, 5)),
            pltpu.SemaphoreType.DMA((2, STEPS, len(DIRS))),
            pltpu.SemaphoreType.DMA((2, STEPS, len(DIRS))),
        ],
        compiler_params=pltpu.CompilerParams(
            collective_id=0, has_side_effects=True, vmem_limit_bytes=40000000
        ),
    )(*[pltpu.with_memory_space_constraint(v, pltpu.HBM) for v in args])


def solution(mesh):
    in_specs = (
        P(None, None, "gx", "gy", None),
        P(None, None, "gx", "gy", None),
        P(None, None, "gx", "gy", None),
        P(None, "gx", "gy", None),
        P(None, "gx", "gy", None),
        P(),
    )
    out_specs = P(None, None, "gx", "gy", None)
    return jax.shard_map(local, mesh=mesh, in_specs=in_specs, out_specs=out_specs, check_vma=False)
```

```python
import functools

import jax
import jax.numpy as jnp
from jax import lax
from jax.experimental import pallas as pl
from jax.experimental.pallas import tpu as pltpu
from jax.sharding import PartitionSpec as P

STEPS = 3
RIDGE = 0.5
F32 = jnp.float32
NS = 10
ND = 6
DIRS = ((-1, 0), (1, 0), (0, -1), (0, 1), (-1, -1), (-1, 1), (1, -1), (1, 1))


def pad8(v):
    return (v + 7) // 8 * 8


def cross(a, b):
    return [
        a[1] * b[2] - a[2] * b[1],
        a[2] * b[0] - a[0] * b[2],
        a[0] * b[1] - a[1] * b[0],
    ]


def translate_static(m, axis):
    n, x, y, z, xx, yy, zz, xy, xz, yz = m
    if axis == 0:
        return [n, x + n, y, z, xx + (x + x) + n, yy, zz, xy + y, xz + z, yz]
    if axis == 1:
        return [n, x, y + n, z, xx, yy + (y + y) + n, zz, xy + x, xz, yz + z]
    return [n, x, y, z + n, xx, yy, zz + (z + z) + n, xy, xz + x, yz + y]


def translate_dynamic(m, axis):
    wx, wy, wz, lx, ly, lz = m
    if axis == 0:
        return [wx, wy, wz, lx, ly - wz, lz + wy]
    if axis == 1:
        return [wx, wy, wz, lx + wz, ly, lz - wx]
    return [wx, wy, wz, lx - wy, ly + wx, lz]


def kernel(
    shift_h, pos_h, vel_h, th_h, off_h, occ_h, res,
    shift_ref, pos, vel, th, off, occ, code, grp, upd, made, est, edy,
    sx_s, sy_s, sc_s, rx_s, ry_s, rc_s, sx_d, sy_d, sc_d, rx_d, ry_d, rc_d,
    in_sem, row_sem, send_sem, recv_sem,
):
    slots, rows, cols, depth = off.shape
    gx, gy = lax.axis_index("gx"), lax.axis_index("gy")
    nx, ny = lax.axis_size("gx"), lax.axis_size("gy")

    def device(dx, dy):
        return (lax.rem(gx + dx + nx, nx), lax.rem(gy + dy + ny, ny))

    shift_load = pltpu.make_async_copy(shift_h, shift_ref, in_sem.at[0])
    shift_load.start()
    lead = lax.rem(gx, 2)
    lead_row, lead_half, lead_edge = lead * (rows - 1), 1 - lead, lead * rows
    tail_row, tail_half, tail_edge = rows - 1 - lead_row, lead, rows - lead_edge
    loads = []
    for k, r in enumerate([lead_row, tail_row][: min(rows, 2)] + list(range(1, rows - 1))):
        pairs = (
            (off_h.at[:, r], off.at[:, r]),
            (occ_h.at[:, r], occ.at[:, r]),
            (pos_h.at[:, :, r], pos.at[:, :, r]),
            (th_h.at[:, :, r], th.at[:, :, r]),
            (vel_h.at[:, :, r], vel.at[:, :, r]),
        )
        loads.append(
            [pltpu.make_async_copy(a, b, row_sem.at[k, i]) for i, (a, b) in enumerate(pairs)]
        )
        for copy in loads[k]:
            copy.start()

    def wait_loads(wanted):
        for copy in wanted:
            copy.wait()

    barrier = pltpu.get_barrier_semaphore()
    for dx, dy in DIRS:
        pl.semaphore_signal(
            barrier, inc=1, device_id=device(dx, dy), device_id_type=pl.DeviceIdType.MESH
        )

    yb, zb = cols // 8, depth // 128
    blocks = yb * zb
    edges = [(0, 1), (rows - 1, 0)]
    second = [(r, h) for r in range(rows) for h in range(2) if (r, h) not in edges]

    def place(r, index):
        y = pl.multiple_of((index // zb) * 8, 8)
        z = pl.multiple_of((index % zb) * 128, 128)
        return r, pl.ds(y, 8), pl.ds(z, 128)

    def accumulate(at, base, wanted, make_terms, new=False):
        total = None
        for m in range(slots):
            if new:
                moved = jnp.bitwise_xor(off[(m,) + at], shift_ref[0])
                own = jnp.where(occ[(m,) + at] == 1, moved, 8)
                code[(m,) + at] = own
            else:
                own = code[(m,) + at]
            terms = make_terms(m)
            picked = []
            for c in wanted:
                mask = own == c
                picked.append([jnp.where(mask, t, 0.0) for t in terms])
            if total is None:
                total = picked
            else:
                total = [[a + b for a, b in zip(u, v)] for u, v in zip(total, picked)]
        for c, values in zip(wanted, total):
            for k, value in enumerate(values):
                grp[(base + k, c) + at] = value

    def point(m, at):
        return [pos[(k, m) + at] for k in range(3)]

    def codes_of(h):
        return [4 * h + c for c in range(4)]

    def shifted(s):
        return jnp.bitwise_xor(shift_ref[s], shift_ref[0])

    def static_sums(r, h, new=False):
        def body(index, carry):
            at = place(r, index)

            def terms(m):
                x, y, z = point(m, at)
                return [1.0, x, y, z, x * x, y * y, z * z, x * y, x * z, y * z]

            accumulate(at, 0, codes_of(h), terms, new)
            return carry

        lax.fori_loop(0, blocks, body, 0)

    def flow_sums(step, r, wanted):
        def body(index, carry):
            at = place(r, index)

            def terms(m):
                now = [th[(k, (m + step) % slots) + at] for k in range(3)]
                if step == 0:
                    before = [vel[(k, m) + at] for k in range(3)]
                else:
                    before = [th[(k, (m + step - 1) % slots) + at] for k in range(3)]
                flow = [a - b for a, b in zip(before, now)]
                return flow + cross(point(m, at), flow)

            accumulate(at, NS + ND * step, wanted, terms)
            return carry

        lax.fori_loop(0, blocks, body, 0)

    sub = lax.broadcasted_iota(jnp.int32, (cols, depth), 0)

    def build(load, translate, count, ext, sx, sy, sc, edges):
        def merged(e, by):
            halves = []
            for bz in range(2):
                parts = []
                if e > 0:
                    parts.append(load(2 * by + bz, e - 1))
                if e < rows:
                    parts.append(translate(load(4 + 2 * by + bz, e), 0))
                halves.append(parts[0] if len(parts) == 1 else [a + b for a, b in zip(*parts)])
            high = [pltpu.roll(v, depth - 1, 1) for v in translate(halves[1], 2)]
            return [a + b for a, b in zip(halves[0], high)]

        for e in edges:
            low = merged(e, 0)
            high = translate(merged(e, 1), 1)
            for v in range(count):
                moved = pltpu.roll(high[v], cols - 1, 0)
                main = low[v] + jnp.where(sub == cols - 1, 0.0, moved)
                rim, last = high[v][0:1], main[cols - 1 : cols]
                ext[v, e, 0:cols] = main
                ext[v, e, cols : cols + 1] = rim
                for side, row in ((0, 0), (1, rows)):
                    if e == row:
                        sx[side, v * cols : (v + 1) * cols] = main
                        sx[side, count * cols + v : count * cols + v + 1] = rim
                        if sc is not None:
                            sc[2 * side, v : v + 1] = rim
                            sc[2 * side + 1, v : v + 1] = last
                sy[0, e * count + v : e * count + v + 1] = rim
                sy[1, e * count + v : e * count + v + 1] = last

    def copies(sx, sy, sc, rx, ry, rc, kind, step):
        out = []
        for k, (dx, dy) in enumerate(DIRS if sc is not None else DIRS[:4]):
            if dy == 0:
                src, dst = sx.at[k], rx.at[k]
            elif dx == 0:
                src, dst = sy.at[k - 2], ry.at[k - 2]
            else:
                src, dst = sc.at[k - 4], rc.at[k - 4]
            out.append(
                pltpu.make_async_remote_copy(
                    src_ref=src, dst_ref=dst,
                    send_sem=send_sem.at[kind, step, k],
                    recv_sem=recv_sem.at[kind, step, k],
                    device_id=device(dx, dy),
                    device_id_type=pl.DeviceIdType.MESH,
                )
            )
        return out

    def absorb_sides(count, ext, ry, rc, sx, sent, wanted):
        for copy in sent:
            copy.wait_recv()
        for v in range(count):
            for e in wanted:
                for side, row in ((0, cols - 1), (1, cols)):
                    extra = ry[side, e * count + v : e * count + v + 1]
                    if rc is not None and e == rows:
                        extra = extra + rc[side, v : v + 1]
                    if rc is not None and e == 0:
                        extra = extra + rc[2 + side, v : v + 1]
                    ext[v, e, row : row + 1] += extra
                if sx is not None and e in (0, rows):
                    for side, edge in ((0, 0), (1, rows)):
                        if e == edge:
                            at = v * cols + cols - 1
                            sx[side, at : at + 1] = ext[v, e, cols - 1 : cols]
                            at = count * cols + v
                            sx[side, at : at + 1] = ext[v, e, cols : cols + 1]

    def absorb_edges(count, ext, rx, sent):
        for copy in sent:
            copy.wait_recv()
        for v in range(count):
            for side, e in ((0, rows), (1, 0)):
                ext[v, e, 0:cols] += rx[side, v * cols : (v + 1) * cols]
                ext[v, e, cols : cols + 1] += rx[side, count * cols + v : count * cols + v + 1]

    def static_solve(ext):
        for e in range(rows + 1):
            n, sx, sy, sz, xx, yy, zz, xy, xz, yz = [ext[v, e] for v in range(NS)]
            inv = 1.0 / jnp.maximum(n, 1.0)
            cx, cy, cz = sx * inv, sy * inv, sz * inv
            mxx, myy, mzz = xx - sx * cx, yy - sy * cy, zz - sz * cz
            kxy, kxz, kyz = sx * cy - xy, sx * cz - xz, sy * cz - yz
            kxx = myy + mzz + RIDGE
            kyy = mxx + mzz + RIDGE
            kzz = mxx + myy + RIDGE
            axx = kyy * kzz - kyz * kyz
            ayy = kxx * kzz - kxz * kxz
            azz = kxx * kyy - kxy * kxy
            axy = kxz * kyz - kxy * kzz
            axz = kxy * kyz - kxz * kyy
            ayz = kxy * kxz - kxx * kyz
            scale = 1.0 / (kxx * axx + kxy * axy + kxz * axz)
            done = [inv, cx, cy, cz] + [a * scale for a in (axx, ayy, azz, axy, axz, ayz)]
            for v in range(NS):
                ext[v, e] = done[v]

    def table(ext, dyn, e):
        inv, cx, cy, cz, ixx, iyy, izz, ixy, ixz, iyz = [ext[v, e] for v in range(NS)]
        flow = [dyn[v, e] for v in range(3)]
        centre = [cx, cy, cz]
        tq = [dyn[3 + k, e] - t for k, t in enumerate(cross(centre, flow))]
        spin = [
            ixx * tq[0] + ixy * tq[1] + ixz * tq[2],
            ixy * tq[0] + iyy * tq[1] + iyz * tq[2],
            ixz * tq[0] + iyz * tq[1] + izz * tq[2],
        ]
        base = [f * inv - t for f, t in zip(flow, cross(spin, centre))]
        values = base + spin
        straight = [v[0:cols] for v in values]
        moved = [
            jnp.where(
                sub == 0,
                jnp.broadcast_to(v[cols : cols + 1], (cols, depth)),
                pltpu.roll(v[0:cols], 1, 0),
            )
            for v in values
        ]
        for by, plain in ((0, straight), (1, moved)):
            for v in range(ND):
                made[e, by, 0, v] = plain[v]
                made[e, by, 1, v] = pltpu.roll(plain[v], 1, 1)

    def solve_half(step, r, h):
        delta = shifted(step)
        for c in range(4):
            want = 4 * h + c
            a0, a1, a2, s0, s1, s2 = [made[r - h + 1, c // 2, c % 2, v] for v in range(ND)]
            if c % 2:
                a0, a1 = a0 + s1, a1 - s0
            if c // 2:
                a0, a2 = a0 - s2, a2 + s0
            if not isinstance(h, int):
                side = lax.convert_element_type(h, F32)
                a1, a2 = a1 + side * s2, a2 - side * s1
            elif h:
                a1, a2 = a1 + s2, a2 - s1
            if step == STEPS - 1:
                done = [a0, a1, a2, s0, s1, s2]
            else:
                own = jnp.bitwise_xor(delta, want)
                n, x, y, z, xx, yy, zz, xy, xz, yz = [grp[v, own, r] for v in range(NS)]
                turn = cross([s0, s1, s2], [x, y, z])
                arm = cross([x, y, z], [a0, a1, a2])
                done = [
                    n * a0 + turn[0],
                    n * a1 + turn[1],
                    n * a2 + turn[2],
                    arm[0] + (yy + zz) * s0 - xy * s1 - xz * s2,
                    arm[1] + (xx + zz) * s1 - xy * s0 - yz * s2,
                    arm[2] + (xx + yy) * s2 - xz * s0 - yz * s1,
                ]
            for v in range(ND):
                upd[v, want, r] = done[v]

    last_step = STEPS - 1
    written = set()

    def final_half(r, h):
        delta = shifted(last_step)
        fresh = r not in written
        written.add(r)

        def body(index, carry):
            at = place(r, index)
            leaf = [[upd[(v, 4 * h + c) + at] for c in range(4)] for v in range(ND)]
            for m in range(slots):
                own = jnp.bitwise_xor(code[(m,) + at], delta)
                one = jnp.bitwise_and(own, 1) == 1
                two = jnp.bitwise_and(own, 2) == 2
                mine = jnp.bitwise_and(own, 12) == 4 * h
                picked = [
                    jnp.where(two, jnp.where(one, l[3], l[2]), jnp.where(one, l[1], l[0]))
                    for l in leaf
                ]
                turn = cross(picked[3:], point(m, at))
                for k in range(3):
                    hot = th[(k, (m + last_step) % slots) + at]
                    old = 0.0 if fresh else res[(k, m) + at]
                    res[(k, m) + at] = jnp.where(mine, hot + picked[k] + turn[k], old)
            return carry

        lax.fori_loop(0, blocks, body, 0)

    def load_static(step):
        delta = shifted(step)

        def load(want, r):
            own = want if step == 0 else jnp.bitwise_xor(delta, want)
            return [grp[v, own, r] for v in range(NS)]

        return load

    def load_dynamic(step):
        delta = shifted(step)

        def load(want, r):
            own = want if step == 0 else jnp.bitwise_xor(delta, want)
            values = [grp[NS + ND * step + v, own, r] for v in range(ND)]
            if step:
                last = jnp.bitwise_xor(own, shifted(step - 1))
                values = [a + upd[v, last, r] for v, a in enumerate(values)]
            return values

        return load

    tips = [(sc_s.at[s], rc_s.at[s]) if s + 1 < STEPS else (None, None) for s in range(STEPS)]
    static_sent = [
        copies(sx_s.at[s], sy_s.at[s], tips[s][0], rx_s.at[s], ry_s.at[s], tips[s][1], 0, s)
        for s in range(STEPS)
    ]
    dynamic_sent = [
        copies(sx_d.at[s], sy_d.at[s], sc_d.at[s], rx_d.at[s], ry_d.at[s], rc_d.at[s], 1, s)
        for s in range(STEPS)
    ]
    groups = {0: (0, 4, 5), rows: (1, 6, 7)}

    def send_edge(sent, e):
        for k in groups[e]:
            if k < len(sent):
                sent[k].start()

    def send_sides(sent):
        sent[2].start()
        sent[3].start()

    def build_static(s, edges):
        build(
            load_static(s), translate_static, NS, est.at[s],
            sx_s.at[s], sy_s.at[s], tips[s][0], edges,
        )

    def build_dynamic(s, edges):
        build(
            load_dynamic(s), translate_dynamic, ND, edy,
            sx_d.at[s], sy_d.at[s], sc_d.at[s], edges,
        )

    inner, every = range(1, rows), range(rows + 1)

    def begin_static(s):
        build_static(s, every)
        send_sides(static_sent[s])

    def send_static(s):
        if tips[s][1] is None:
            absorb_sides(NS, est.at[s], ry_s.at[s], None, sx_s.at[s], static_sent[s][2:], every)
        for e in (0, rows):
            send_edge(static_sent[s], e)

    def finish_static(s):
        absorb_edges(NS, est.at[s], rx_s.at[s], static_sent[s][:2])
        if tips[s][1] is not None:
            absorb_sides(
                NS, est.at[s], ry_s.at[s], tips[s][1], None, static_sent[s][2:], every
            )
        static_solve(est.at[s])

    def absorb_inner(s):
        sent = dynamic_sent[s][2:4]
        absorb_sides(ND, edy, ry_d.at[s], None, None, sent, inner)

    def absorb_outer(s):
        sent = dynamic_sent[s]
        absorb_edges(ND, edy, rx_d.at[s], sent[:2])
        absorb_sides(ND, edy, ry_d.at[s], rc_d.at[s], None, sent[4:], (0, rows))

    def at_edge(edge, act):
        for e in (0, rows):
            pl.when(edge == e)(functools.partial(act, e))

    def static_edge(s, e):
        build_static(s, [e])
        send_edge(static_sent[s], e)

    def dynamic_edge(s, e):
        build_dynamic(s, [e])
        send_edge(dynamic_sent[s], e)

    shift_load.wait()
    wait_loads(loads[0][:3])
    static_sums(lead_row, lead_half, True)
    pl.semaphore_wait(barrier, len(DIRS))
    at_edge(lead_edge, functools.partial(static_edge, 0))
    wait_loads(loads[0][3:])
    flow_sums(0, lead_row, codes_of(lead_half))
    at_edge(lead_edge, functools.partial(dynamic_edge, 0))
    for group in loads[1:]:
        wait_loads(group)
    static_sums(tail_row, tail_half, True)
    at_edge(tail_edge, functools.partial(static_edge, 0))
    flow_sums(0, tail_row, codes_of(tail_half))
    at_edge(tail_edge, functools.partial(dynamic_edge, 0))
    for r, h in second:
        static_sums(r, h, 0 < r < rows - 1 and h == 0)
    build_static(0, inner)
    send_sides(static_sent[0])
    for r, h in second:
        flow_sums(0, r, codes_of(h))
    build_dynamic(0, inner)
    send_sides(dynamic_sent[0])
    begin_static(1)
    for r in range(rows):
        flow_sums(1, r, range(8))
        if r == 0:
            send_static(1)
    begin_static(2)
    finish_static(0)
    for s in range(STEPS):
        absorb_inner(s)
        for e in inner:
            table(est.at[s], edy, e)
        for r, h in second:
            solve_half(s, r, h)
        if s == last_step:
            for r, h in second:
                final_half(r, h)
        absorb_outer(s)
        table(est.at[s], edy, lead_edge)
        solve_half(s, lead_row, lead_half)
        if s < last_step:
            at_edge(lead_edge, functools.partial(dynamic_edge, s + 1))
        table(est.at[s], edy, tail_edge)
        solve_half(s, tail_row, tail_half)
        if s < last_step:
            at_edge(tail_edge, functools.partial(dynamic_edge, s + 1))
            build_dynamic(s + 1, inner)
            send_sides(dynamic_sent[s + 1])
            if s == 0:
                for r in range(rows):
                    flow_sums(2, r, range(8))
                    if r == 0:
                        send_static(2)
            finish_static(s + 1)
    for r, h in edges:
        final_half(r, h)
    for group in static_sent + dynamic_sent:
        for copy in group:
            copy.wait_send()


def local(positions, velocities, thermal, offsets, occupancy, shift_codes):
    args = (shift_codes, positions, velocities, thermal, offsets, occupancy)
    slots, rows, cols, depth = offsets.shape
    full = (3, slots, rows, cols, depth)
    plane = (slots, rows, cols, depth)

    def faces(count, tip_steps):
        wide = pltpu.VMEM((STEPS, 2, count * cols + pad8(count), depth), F32)
        thin = pltpu.VMEM((STEPS, 2, pad8((rows + 1) * count), depth), F32)
        tips = pltpu.VMEM((tip_steps, 4, pad8(count), depth), F32)
        return [wide, thin, tips] * 2

    hbm = pl.BlockSpec(memory_space=pltpu.HBM)
    return pl.pallas_call(
        kernel,
        out_shape=pltpu.VMEM(full, F32),
        in_specs=[hbm] * 6,
        out_specs=pl.BlockSpec(memory_space=pltpu.VMEM),
        scratch_shapes=[
            pltpu.SMEM((STEPS,), jnp.int32),
            pltpu.VMEM(full, F32),
            pltpu.VMEM(full, F32),
            pltpu.VMEM(full, F32),
            pltpu.VMEM(plane, jnp.int32),
            pltpu.VMEM(plane, jnp.int32),
            pltpu.VMEM(plane, jnp.int32),
            pltpu.VMEM((NS + ND * STEPS, 8, rows, cols, depth), F32),
            pltpu.VMEM((ND, 8, rows, cols, depth), F32),
            pltpu.VMEM((rows + 1, 2, 2, ND, cols, depth), F32),
            pltpu.VMEM((STEPS, NS, rows + 1, cols + 8, depth), F32),
            pltpu.VMEM((ND, rows + 1, cols + 8, depth), F32),
            *faces(NS, STEPS - 1),
            *faces(ND, STEPS),
            pltpu.SemaphoreType.DMA((1,)),
            pltpu.SemaphoreType.DMA((rows, 5)),
            pltpu.SemaphoreType.DMA((2, STEPS, len(DIRS))),
            pltpu.SemaphoreType.DMA((2, STEPS, len(DIRS))),
        ],
        compiler_params=pltpu.CompilerParams(
            collective_id=0, has_side_effects=True, vmem_limit_bytes=40000000
        ),
    )(*[pltpu.with_memory_space_constraint(v, pltpu.HBM) for v in args])


def solution(mesh):
    in_specs = (
        P(None, None, "gx", "gy", None),
        P(None, None, "gx", "gy", None),
        P(None, None, "gx", "gy", None),
        P(None, "gx", "gy", None),
        P(None, "gx", "gy", None),
        P(),
    )
    out_specs = P(None, None, "gx", "gy", None)
    return jax.shard_map(local, mesh=mesh, in_specs=in_specs, out_specs=out_specs, check_vma=False)
```

```python
import functools

import jax
import jax.numpy as jnp
from jax import lax
from jax.experimental import pallas as pl
from jax.experimental.pallas import tpu as pltpu
from jax.sharding import PartitionSpec as P

STEPS = 3
RIDGE = 0.5
F32 = jnp.float32
NS = 10
ND = 6
DIRS = ((-1, 0), (1, 0), (0, -1), (0, 1), (-1, -1), (-1, 1), (1, -1), (1, 1))


def pad8(v):
    return (v + 7) // 8 * 8


def cross(a, b):
    return [
        a[1] * b[2] - a[2] * b[1],
        a[2] * b[0] - a[0] * b[2],
        a[0] * b[1] - a[1] * b[0],
    ]


def translate_static(m, axis):
    n, x, y, z, xx, yy, zz, xy, xz, yz = m
    if axis == 0:
        return [n, x + n, y, z, xx + (x + x) + n, yy, zz, xy + y, xz + z, yz]
    if axis == 1:
        return [n, x, y + n, z, xx, yy + (y + y) + n, zz, xy + x, xz, yz + z]
    return [n, x, y, z + n, xx, yy, zz + (z + z) + n, xy, xz + x, yz + y]


def translate_dynamic(m, axis):
    wx, wy, wz, lx, ly, lz = m
    if axis == 0:
        return [wx, wy, wz, lx, ly - wz, lz + wy]
    if axis == 1:
        return [wx, wy, wz, lx + wz, ly, lz - wx]
    return [wx, wy, wz, lx - wy, ly + wx, lz]


def kernel(
    shift_h, pos_h, vel_h, th_h, off_h, occ_h, res,
    shift_ref, pos, vel, th, off, occ, code, grp, upd, made, est, edy,
    sx_s, sy_s, sc_s, sr_s, rx_s, ry_s, rc_s, rr_s,
    sx_d, sy_d, sc_d, sr_d, rx_d, ry_d, rc_d, rr_d,
    in_sem, row_sem, send_sem, recv_sem,
):
    slots, rows, cols, depth = off.shape
    gx, gy = lax.axis_index("gx"), lax.axis_index("gy")
    nx, ny = lax.axis_size("gx"), lax.axis_size("gy")

    def device(dx, dy):
        return (lax.rem(gx + dx + nx, nx), lax.rem(gy + dy + ny, ny))

    shift_load = pltpu.make_async_copy(shift_h, shift_ref, in_sem.at[0])
    shift_load.start()
    lead = lax.rem(gx, 2)
    lead_row, lead_half, lead_edge = lead * (rows - 1), 1 - lead, lead * rows
    tail_row, tail_half, tail_edge = rows - 1 - lead_row, lead, rows - lead_edge
    yb, zb = cols // 8, depth // 128
    loads = []
    for k, r in enumerate([lead_row, tail_row][: min(rows, 2)] + list(range(1, rows - 1))):
        pairs = []
        for j in range(yb):
            y = pl.ds(8 * j, 8)
            pairs += [
                (off_h.at[:, r, y], off.at[:, r, y]),
                (occ_h.at[:, r, y], occ.at[:, r, y]),
                (pos_h.at[:, :, r, y], pos.at[:, :, r, y]),
            ]
        pairs += [
            (th_h.at[:, :, r], th.at[:, :, r]),
            (vel_h.at[:, :, r], vel.at[:, :, r]),
        ]
        loads.append(
            [pltpu.make_async_copy(a, b, row_sem.at[k, i]) for i, (a, b) in enumerate(pairs)]
        )
        for copy in loads[k]:
            copy.start()

    def wait_loads(wanted):
        for copy in wanted:
            copy.wait()

    barrier = pltpu.get_barrier_semaphore()
    for dx, dy in DIRS:
        pl.semaphore_signal(
            barrier, inc=1, device_id=device(dx, dy), device_id_type=pl.DeviceIdType.MESH
        )

    blocks = yb * zb
    edges = [(0, 1), (rows - 1, 0)]
    second = [(r, h) for r in range(rows) for h in range(2) if (r, h) not in edges]

    def place(r, index):
        y = pl.multiple_of((index // zb) * 8, 8)
        z = pl.multiple_of((index % zb) * 128, 128)
        return r, pl.ds(y, 8), pl.ds(z, 128)

    def accumulate(at, base, wanted, make_terms, new=False):
        total = None
        for m in range(slots):
            if new:
                moved = jnp.bitwise_xor(off[(m,) + at], shift_ref[0])
                own = jnp.where(occ[(m,) + at] == 1, moved, 8)
                code[(m,) + at] = own
            else:
                own = code[(m,) + at]
            terms = make_terms(m)
            picked = []
            for c in wanted:
                mask = own == c
                picked.append([jnp.where(mask, t, 0.0) for t in terms])
            if total is None:
                total = picked
            else:
                total = [[a + b for a, b in zip(u, v)] for u, v in zip(total, picked)]
        for c, values in zip(wanted, total):
            for k, value in enumerate(values):
                grp[(base + k, c) + at] = value

    def point(m, at):
        return [pos[(k, m) + at] for k in range(3)]

    def codes_of(h):
        return [4 * h + c for c in range(4)]

    def shifted(s):
        return jnp.bitwise_xor(shift_ref[s], shift_ref[0])

    def static_sums(r, h, new=False, start=0, stop=blocks):
        def body(index, carry):
            at = place(r, index)

            def terms(m):
                x, y, z = point(m, at)
                return [1.0, x, y, z, x * x, y * y, z * z, x * y, x * z, y * z]

            accumulate(at, 0, codes_of(h), terms, new)
            return carry

        lax.fori_loop(start, stop, body, 0)

    def flow_sums(step, r, wanted):
        def body(index, carry):
            at = place(r, index)

            def terms(m):
                now = [th[(k, (m + step) % slots) + at] for k in range(3)]
                if step == 0:
                    before = [vel[(k, m) + at] for k in range(3)]
                else:
                    before = [th[(k, (m + step - 1) % slots) + at] for k in range(3)]
                flow = [a - b for a, b in zip(before, now)]
                return flow + cross(point(m, at), flow)

            accumulate(at, NS + ND * step, wanted, terms)
            return carry

        lax.fori_loop(0, blocks, body, 0)

    sub = lax.broadcasted_iota(jnp.int32, (cols, depth), 0)

    def put(ref, side, v, row):
        for z in range(zb):
            ref[side, v * zb + z : v * zb + z + 1] = row[:, z * 128 : (z + 1) * 128]

    def add(ext, v, e, row, ref, side):
        for z in range(zb):
            ext[v, e, row : row + 1, z * 128 : (z + 1) * 128] += ref[
                side, v * zb + z : v * zb + z + 1
            ]

    def build(load, translate, count, ext, sx, sy, sc, sr, edges):
        def merged(e, by):
            halves = []
            for bz in range(2):
                parts = []
                if e > 0:
                    parts.append(load(2 * by + bz, e - 1))
                if e < rows:
                    parts.append(translate(load(4 + 2 * by + bz, e), 0))
                halves.append(parts[0] if len(parts) == 1 else [a + b for a, b in zip(*parts)])
            high = [pltpu.roll(v, depth - 1, 1) for v in translate(halves[1], 2)]
            return [a + b for a, b in zip(halves[0], high)]

        for e in edges:
            low = merged(e, 0)
            high = translate(merged(e, 1), 1)
            for v in range(count):
                moved = pltpu.roll(high[v], cols - 1, 0)
                main = low[v] + jnp.where(sub == cols - 1, 0.0, moved)
                rim, last = high[v][0:1], main[cols - 1 : cols]
                ext[v, e, 0:cols] = main
                ext[v, e, cols : cols + 1] = rim
                for side, row in ((0, 0), (1, rows)):
                    if e == row:
                        sx[side, v * cols : (v + 1) * cols] = main
                        put(sr, side, v, rim)
                        if sc is not None:
                            put(sc, 2 * side, v, rim)
                            put(sc, 2 * side + 1, v, last)
                sy[0, e * count + v : e * count + v + 1] = rim
                sy[1, e * count + v : e * count + v + 1] = last

    def copies(sx, sy, sc, sr, rx, ry, rc, rr, kind, step):
        moves = []
        for k, where in enumerate(DIRS[:4]):
            wide = k < 2
            moves.append((where, sx.at[k] if wide else sy.at[k - 2], rx.at[k] if wide else ry.at[k - 2]))
        for k, where in enumerate(DIRS[:2]):
            moves.append((where, sr.at[k], rr.at[k]))
        if sc is not None:
            for k, where in enumerate(DIRS[4:]):
                moves.append((where, sc.at[k], rc.at[k]))
        return [
            pltpu.make_async_remote_copy(
                src_ref=src, dst_ref=dst,
                send_sem=send_sem.at[kind, step, k],
                recv_sem=recv_sem.at[kind, step, k],
                device_id=device(*where),
                device_id_type=pl.DeviceIdType.MESH,
            )
            for k, (where, src, dst) in enumerate(moves)
        ]

    def absorb_sides(count, ext, ry, rc, out, sent, wanted):
        for copy in sent:
            copy.wait_recv()
        for v in range(count):
            for e in wanted:
                for side, row in ((0, cols - 1), (1, cols)):
                    ext[v, e, row : row + 1] += ry[side, e * count + v : e * count + v + 1]
                    if rc is not None and e == rows:
                        add(ext, v, e, row, rc, side)
                    if rc is not None and e == 0:
                        add(ext, v, e, row, rc, 2 + side)
                for side, edge in ((0, 0), (1, rows)):
                    if out is not None and e == edge:
                        at = v * cols + cols - 1
                        out[0][side, at : at + 1] = ext[v, e, cols - 1 : cols]
                        put(out[1], side, v, ext[v, e, cols : cols + 1])

    def absorb_edges(count, ext, rx, rr, sent):
        for copy in sent:
            copy.wait_recv()
        for v in range(count):
            for side, e in ((0, rows), (1, 0)):
                ext[v, e, 0:cols] += rx[side, v * cols : (v + 1) * cols]
                add(ext, v, e, cols, rr, side)

    def static_solve(ext):
        for e in range(rows + 1):
            n, sx, sy, sz, xx, yy, zz, xy, xz, yz = [ext[v, e] for v in range(NS)]
            inv = 1.0 / jnp.maximum(n, 1.0)
            cx, cy, cz = sx * inv, sy * inv, sz * inv
            mxx, myy, mzz = xx - sx * cx, yy - sy * cy, zz - sz * cz
            kxy, kxz, kyz = sx * cy - xy, sx * cz - xz, sy * cz - yz
            kxx = myy + mzz + RIDGE
            kyy = mxx + mzz + RIDGE
            kzz = mxx + myy + RIDGE
            axx = kyy * kzz - kyz * kyz
            ayy = kxx * kzz - kxz * kxz
            azz = kxx * kyy - kxy * kxy
            axy = kxz * kyz - kxy * kzz
            axz = kxy * kyz - kxz * kyy
            ayz = kxy * kxz - kxx * kyz
            scale = 1.0 / (kxx * axx + kxy * axy + kxz * axz)
            done = [inv, cx, cy, cz] + [a * scale for a in (axx, ayy, azz, axy, axz, ayz)]
            for v in range(NS):
                ext[v, e] = done[v]

    def table(ext, dyn, e):
        inv, cx, cy, cz, ixx, iyy, izz, ixy, ixz, iyz = [ext[v, e] for v in range(NS)]
        flow = [dyn[v, e] for v in range(3)]
        centre = [cx, cy, cz]
        tq = [dyn[3 + k, e] - t for k, t in enumerate(cross(centre, flow))]
        spin = [
            ixx * tq[0] + ixy * tq[1] + ixz * tq[2],
            ixy * tq[0] + iyy * tq[1] + iyz * tq[2],
            ixz * tq[0] + iyz * tq[1] + izz * tq[2],
        ]
        base = [f * inv - t for f, t in zip(flow, cross(spin, centre))]
        values = base + spin
        straight = [v[0:cols] for v in values]
        moved = [
            jnp.where(
                sub == 0,
                jnp.broadcast_to(v[cols : cols + 1], (cols, depth)),
                pltpu.roll(v[0:cols], 1, 0),
            )
            for v in values
        ]
        for by, plain in ((0, straight), (1, moved)):
            for v in range(ND):
                made[e, by, 0, v] = plain[v]
                made[e, by, 1, v] = pltpu.roll(plain[v], 1, 1)

    def solve_half(step, r, h):
        delta = shifted(step)
        for c in range(4):
            want = 4 * h + c
            a0, a1, a2, s0, s1, s2 = [made[r - h + 1, c // 2, c % 2, v] for v in range(ND)]
            if c % 2:
                a0, a1 = a0 + s1, a1 - s0
            if c // 2:
                a0, a2 = a0 - s2, a2 + s0
            if not isinstance(h, int):
                side = lax.convert_element_type(h, F32)
                a1, a2 = a1 + side * s2, a2 - side * s1
            elif h:
                a1, a2 = a1 + s2, a2 - s1
            if step == STEPS - 1:
                done = [a0, a1, a2, s0, s1, s2]
            else:
                own = jnp.bitwise_xor(delta, want)
                n, x, y, z, xx, yy, zz, xy, xz, yz = [grp[v, own, r] for v in range(NS)]
                turn = cross([s0, s1, s2], [x, y, z])
                arm = cross([x, y, z], [a0, a1, a2])
                done = [
                    n * a0 + turn[0],
                    n * a1 + turn[1],
                    n * a2 + turn[2],
                    arm[0] + (yy + zz) * s0 - xy * s1 - xz * s2,
                    arm[1] + (xx + zz) * s1 - xy * s0 - yz * s2,
                    arm[2] + (xx + yy) * s2 - xz * s0 - yz * s1,
                ]
            for v in range(ND):
                upd[v, want, r] = done[v]

    last_step = STEPS - 1
    written = set()

    def final_half(r, h):
        delta = shifted(last_step)
        fresh = r not in written
        written.add(r)

        def body(index, carry):
            at = place(r, index)
            leaf = [[upd[(v, 4 * h + c) + at] for c in range(4)] for v in range(ND)]
            for m in range(slots):
                own = jnp.bitwise_xor(code[(m,) + at], delta)
                one = jnp.bitwise_and(own, 1) == 1
                two = jnp.bitwise_and(own, 2) == 2
                mine = jnp.bitwise_and(own, 12) == 4 * h
                picked = [
                    jnp.where(two, jnp.where(one, l[3], l[2]), jnp.where(one, l[1], l[0]))
                    for l in leaf
                ]
                turn = cross(picked[3:], point(m, at))
                for k in range(3):
                    hot = th[(k, (m + last_step) % slots) + at]
                    old = 0.0 if fresh else res[(k, m) + at]
                    res[(k, m) + at] = jnp.where(mine, hot + picked[k] + turn[k], old)
            return carry

        lax.fori_loop(0, blocks, body, 0)

    def load_static(step):
        delta = shifted(step)

        def load(want, r):
            own = want if step == 0 else jnp.bitwise_xor(delta, want)
            return [grp[v, own, r] for v in range(NS)]

        return load

    def load_dynamic(step):
        delta = shifted(step)

        def load(want, r):
            own = want if step == 0 else jnp.bitwise_xor(delta, want)
            values = [grp[NS + ND * step + v, own, r] for v in range(ND)]
            if step:
                last = jnp.bitwise_xor(own, shifted(step - 1))
                values = [a + upd[v, last, r] for v, a in enumerate(values)]
            return values

        return load

    tips = [(sc_s.at[s], rc_s.at[s]) if s + 1 < STEPS else (None, None) for s in range(STEPS)]
    static_sent = [
        copies(
            sx_s.at[s], sy_s.at[s], tips[s][0], sr_s.at[s],
            rx_s.at[s], ry_s.at[s], tips[s][1], rr_s.at[s], 0, s,
        )
        for s in range(STEPS)
    ]
    dynamic_sent = [
        copies(
            sx_d.at[s], sy_d.at[s], sc_d.at[s], sr_d.at[s],
            rx_d.at[s], ry_d.at[s], rc_d.at[s], rr_d.at[s], 1, s,
        )
        for s in range(STEPS)
    ]
    groups = {0: (0, 4, 6, 7), rows: (1, 5, 8, 9)}

    def send_edge(sent, e):
        for k in groups[e]:
            if k < len(sent):
                sent[k].start()

    def send_sides(sent):
        sent[2].start()
        sent[3].start()

    def build_static(s, edges):
        build(
            load_static(s), translate_static, NS, est.at[s],
            sx_s.at[s], sy_s.at[s], tips[s][0], sr_s.at[s], edges,
        )

    def build_dynamic(s, edges):
        build(
            load_dynamic(s), translate_dynamic, ND, edy,
            sx_d.at[s], sy_d.at[s], sc_d.at[s], sr_d.at[s], edges,
        )

    inner, every = range(1, rows), range(rows + 1)

    def begin_static(s):
        build_static(s, every)
        send_sides(static_sent[s])

    def send_static(s):
        if tips[s][1] is None:
            out = (sx_s.at[s], sr_s.at[s])
            absorb_sides(NS, est.at[s], ry_s.at[s], None, out, static_sent[s][2:4], every)
        for e in (0, rows):
            send_edge(static_sent[s], e)

    def finish_static(s):
        sent = static_sent[s]
        absorb_edges(NS, est.at[s], rx_s.at[s], rr_s.at[s], sent[:2] + sent[4:6])
        if tips[s][1] is not None:
            late = sent[2:4] + sent[6:]
            absorb_sides(NS, est.at[s], ry_s.at[s], tips[s][1], None, late, every)
        static_solve(est.at[s])

    def absorb_inner(s):
        sent = dynamic_sent[s][2:4]
        absorb_sides(ND, edy, ry_d.at[s], None, None, sent, inner)

    def absorb_outer(s):
        sent = dynamic_sent[s]
        absorb_edges(ND, edy, rx_d.at[s], rr_d.at[s], sent[:2] + sent[4:6])
        absorb_sides(ND, edy, ry_d.at[s], rc_d.at[s], None, sent[6:], (0, rows))

    def at_edge(edge, act):
        for e in (0, rows):
            pl.when(edge == e)(functools.partial(act, e))

    def static_edge(s, e):
        build_static(s, [e])
        send_edge(static_sent[s], e)

    def dynamic_edge(s, e):
        build_dynamic(s, [e])
        send_edge(dynamic_sent[s], e)

    shift_load.wait()
    for j in range(yb):
        wait_loads(loads[0][3 * j : 3 * j + 3])
        static_sums(lead_row, lead_half, True, j * zb, j * zb + zb)
    pl.semaphore_wait(barrier, len(DIRS))
    at_edge(lead_edge, functools.partial(static_edge, 0))
    wait_loads(loads[0][3 * yb :])
    flow_sums(0, lead_row, codes_of(lead_half))
    at_edge(lead_edge, functools.partial(dynamic_edge, 0))
    for group in loads[1:]:
        wait_loads(group)
    static_sums(tail_row, tail_half, True)
    at_edge(tail_edge, functools.partial(static_edge, 0))
    flow_sums(0, tail_row, codes_of(tail_half))
    at_edge(tail_edge, functools.partial(dynamic_edge, 0))
    for r, h in second:
        static_sums(r, h, 0 < r < rows - 1 and h == 0)
    build_static(0, inner)
    send_sides(static_sent[0])
    for r, h in second:
        flow_sums(0, r, codes_of(h))
    build_dynamic(0, inner)
    send_sides(dynamic_sent[0])
    begin_static(1)
    for r in range(rows):
        flow_sums(1, r, range(8))
        if r == 0:
            send_static(1)
    begin_static(2)
    finish_static(0)
    for s in range(STEPS):
        absorb_inner(s)
        for e in inner:
            table(est.at[s], edy, e)
        for r, h in second:
            solve_half(s, r, h)
        if s == last_step:
            for r, h in second:
                final_half(r, h)
        absorb_outer(s)
        table(est.at[s], edy, lead_edge)
        solve_half(s, lead_row, lead_half)
        if s < last_step:
            at_edge(lead_edge, functools.partial(dynamic_edge, s + 1))
        table(est.at[s], edy, tail_edge)
        solve_half(s, tail_row, tail_half)
        if s < last_step:
            at_edge(tail_edge, functools.partial(dynamic_edge, s + 1))
            build_dynamic(s + 1, inner)
            send_sides(dynamic_sent[s + 1])
            if s == 0:
                for r in range(rows):
                    flow_sums(2, r, range(8))
                    if r == 0:
                        send_static(2)
            finish_static(s + 1)
    for r, h in edges:
        final_half(r, h)
    for group in static_sent + dynamic_sent:
        for copy in group:
            copy.wait_send()


def local(positions, velocities, thermal, offsets, occupancy, shift_codes):
    args = (shift_codes, positions, velocities, thermal, offsets, occupancy)
    slots, rows, cols, depth = offsets.shape
    full = (3, slots, rows, cols, depth)
    plane = (slots, rows, cols, depth)

    def faces(count, tip_steps):
        lines = pad8(count * (depth // 128))
        wide = pltpu.VMEM((STEPS, 2, pad8(count * cols), depth), F32)
        thin = pltpu.VMEM((STEPS, 2, pad8((rows + 1) * count), depth), F32)
        tips = pltpu.VMEM((tip_steps, 4, lines, 128), F32)
        rims = pltpu.VMEM((STEPS, 2, lines, 128), F32)
        return [wide, thin, tips, rims] * 2

    hbm = pl.BlockSpec(memory_space=pltpu.HBM)
    return pl.pallas_call(
        kernel,
        out_shape=pltpu.VMEM(full, F32),
        in_specs=[hbm] * 6,
        out_specs=pl.BlockSpec(memory_space=pltpu.VMEM),
        scratch_shapes=[
            pltpu.SMEM((STEPS,), jnp.int32),
            pltpu.VMEM(full, F32),
            pltpu.VMEM(full, F32),
            pltpu.VMEM(full, F32),
            pltpu.VMEM(plane, jnp.int32),
            pltpu.VMEM(plane, jnp.int32),
            pltpu.VMEM(plane, jnp.int32),
            pltpu.VMEM((NS + ND * STEPS, 8, rows, cols, depth), F32),
            pltpu.VMEM((ND, 8, rows, cols, depth), F32),
            pltpu.VMEM((rows + 1, 2, 2, ND, cols, depth), F32),
            pltpu.VMEM((STEPS, NS, rows + 1, cols + 8, depth), F32),
            pltpu.VMEM((ND, rows + 1, cols + 8, depth), F32),
            *faces(NS, STEPS - 1),
            *faces(ND, STEPS),
            pltpu.SemaphoreType.DMA((1,)),
            pltpu.SemaphoreType.DMA((rows, 3 * (cols // 8) + 2)),
            pltpu.SemaphoreType.DMA((2, STEPS, len(DIRS) + 2)),
            pltpu.SemaphoreType.DMA((2, STEPS, len(DIRS) + 2)),
        ],
        compiler_params=pltpu.CompilerParams(
            collective_id=0, has_side_effects=True, vmem_limit_bytes=40000000
        ),
    )(*[pltpu.with_memory_space_constraint(v, pltpu.HBM) for v in args])


def solution(mesh):
    in_specs = (
        P(None, None, "gx", "gy", None),
        P(None, None, "gx", "gy", None),
        P(None, None, "gx", "gy", None),
        P(None, "gx", "gy", None),
        P(None, "gx", "gy", None),
        P(),
    )
    out_specs = P(None, None, "gx", "gy", None)
    return jax.shard_map(local, mesh=mesh, in_specs=in_specs, out_specs=out_specs, check_vma=False)
```
